32 devices in a mesh: dp: 8 (over z, x), tp: 4 (over y, core).
Axes of the slice: x: 2, y: 2, z: 4, core: 2. Of those that a mesh axis runs over, the one named last changes fastest.
Arguments:
- queries: bfloat16 [512, 73728], P('dp', 'tp'), may hold values from -32 to 32
- prefix_cache: bfloat16 [8, 576, 1024], P('dp', None, 'tp'), may hold values from -12 to 12
- suffix_cache: bfloat16 [512, 576, 128], P('dp'), may hold values from -48 to 48
- w_uv: bfloat16 [128, 512, 128], P('tp'), may hold values from -1 to 1
- fork_prompt: int32 [512, 1], P('dp'), may hold values from 0 to 7; in each aligned block of 64 rows (0 to 63, 64 to 127, ...) at most 16 rows name the same one
- prompt_slot: int32 [8], replicated, may hold values from 0 to 7, each once
- suffix_len: int32 [512], P('dp'), may hold values from 32 to 128
Outputs:
- attended: bfloat16 [512, 16384], P('dp', 'tp')
The draws below stay inside these ranges and needn't reach their ends.
Inputs may be any that keep to these rules, and one draw needn't show every extreme that they name: `fork_prompt`: among the 64 forks of one index of dp no prompt is named more than 16 times. `prompt_slot`: each slot holds exactly one prompt.
All inputs are finite; a program needn't handle non-finite values.
Results may differ from the reference program's by a relative error of at most 0.033.
Values may be sent and summed in bfloat16 or wider, within the bound.
A program may use at most 128 MiB of HBM per device.

```python
import math
import jax
import jax.numpy as jnp
import numpy as np
from jax import lax

H = 128
R = 512
P_SIZE = 64
V = 128
L = 1024
S = 128
FORK_DEV = 64
MOST = 16
PROMPTS = 8
FORKS = 512


def fork_pair(key):
    base = jax.random.fold_in(key, 7001)
    streams = jax.random.split(base, 2)
    key_width = R + P_SIZE
    suffix = jnp.clip(jax.random.normal(streams[0], (FORKS, key_width, S), jnp.float32), -4.0, 4.0)
    query = jnp.clip(jax.random.normal(streams[1], (FORKS, H, key_width), jnp.float32), -4.0, 4.0)
    suffix = jnp.clip(suffix, -48.0, 48.0)
    query = jnp.clip(query, -32.0, 32.0)
    return (query, suffix)


def draw_queries(key, part):
    query, suffix = fork_pair(key)
    return query.reshape(FORKS, H * (R + P_SIZE)).astype(jnp.bfloat16)


def draw_suffix_cache(key, part):
    query, suffix = fork_pair(key)
    return suffix.astype(jnp.bfloat16)


def draw_prefix_cache(key, part):
    base = jax.random.fold_in(key, 7002)
    streams = jax.random.split(base, 1)
    cache = jnp.clip(jax.random.normal(streams[0], (PROMPTS, R + P_SIZE, L), jnp.float32), -4.0, 4.0)
    return cache.astype(jnp.bfloat16)


def set_ends(values, key, low, high):
    longest = values.shape.index(max(values.shape))
    spots = []
    for shift in (0, 1):
        where = [jax.random.randint(jax.random.fold_in(key, axis), (), 0, length) for axis, length in enumerate(values.shape)]
        where[longest] = (where[longest] + shift) % values.shape[longest]
        spots.append(tuple(where))
    return values.at[spots[0]].set(low).at[spots[1]].set(high)


def shard_levels(stream_key, shape, shards, low, high):
    def one(axis_at, parts):
        steps = jax.random.uniform(jax.random.fold_in(jax.random.fold_in(stream_key, 6), axis_at), (parts,), jnp.float32, low / len(shards), high / len(shards))
        return jnp.repeat(jnp.exp(steps), shape[axis_at] // parts).reshape((-1,) + (1,) * (len(shape) - axis_at - 1))

    level = one(*shards[0])
    for cut in shards[1:]:
        level = level * one(*cut)
    return level


def shared_out(rng, own, number, rows, number_of, top, bound, skew):
    sequence = jax.random.permutation(rng, number_of)
    packed, common = portions_of(number_of, rows * top, bound, skew, True), portions_of(number_of, rows * top, bound, skew, False)
    places = jnp.arange(number_of)

    def named(lengths, rotation):
        used = int((lengths > 0).sum())
        fixed = max(1, used // 4)
        moved = fixed + (places - fixed + rotation * (used - fixed)) % max(1, number_of - fixed)
        return jnp.zeros((number_of,), jnp.int32).at[sequence[jnp.where(places < fixed, places, moved)]].set(jnp.asarray(lengths, jnp.int32))

    lengths = jnp.where(number % 4 == 0, named(packed, number // 4), named(common, number - number // 4 - 1))
    mixed = jax.random.permutation(jax.random.fold_in(own, 3), number_of)
    source_of, sink = mixed[0:number_of // 2 * 2:2], mixed[1:number_of // 2 * 2:2]
    slack = jnp.minimum(lengths[source_of] - 1, bound - lengths[sink]) // 2
    slack = jnp.where((source_of == sequence[0]) | (sink == sequence[0]) | (lengths[sink] == 0), 0, jnp.maximum(slack, 0))
    moved = jax.random.randint(jax.random.fold_in(own, 4), (number_of // 2,), 0, 1 << 20) % (slack + 1)
    lengths = lengths.at[source_of].add(-moved).at[sink].add(moved)
    members = jnp.searchsorted(jnp.cumsum(lengths), jnp.arange(rows * top), side="right").astype(jnp.int32)
    table = members.reshape(top, rows).T
    table = table[jax.random.permutation(jax.random.fold_in(own, 1), rows)]
    rotation = jax.random.randint(jax.random.fold_in(own, 2), (rows, 1), 0, top)
    return jnp.take_along_axis(table, (jnp.arange(top)[None, :] + rotation) % top, axis=1)


def portions_of(amount, total, bound, slope, full):
    weights = [(1 << 20) // math.isqrt(standing ** slope) + 1 for standing in range(1, amount + 1)]
    largest = bound if full else min(bound, max(-(-total // amount), total * weights[0] // sum(weights)))
    least = 1 if total - largest >= amount - 1 else 0
    counts, rest = [largest] + [least] * (amount - 1), total - largest - least * (amount - 1)
    while rest > 0:
        movable = [i for i in range(1, amount) if counts[i] < largest] or [i for i in range(1, amount) if counts[i] < bound]
        pool, budget = sum([weights[i] for i in movable]), rest
        for i in movable:
            more = min(bound - counts[i], max(1, budget * weights[i] // pool), rest)
            counts[i] = counts[i] + more
            rest = rest - more
    return np.array(counts)


def normal_values(own_key, dims, scale, most, pieces=(), kind=jnp.bfloat16):
    values = scale * jax.random.normal(own_key, dims, jnp.float32)
    if pieces:
        values = values * shard_levels(own_key, dims, pieces, -0.22, 0.18)
    return jnp.clip(values, -most, most).astype(kind)


def setup_inputs(seed: int = 0) -> dict:
    arg_keys = jax.random.split(jax.random.key(seed), 8)
    queries = draw_queries(jax.random.fold_in(arg_keys[7], 71), 0)
    prefix_cache = draw_prefix_cache(jax.random.fold_in(arg_keys[7], 71), 0)
    suffix_cache = draw_suffix_cache(jax.random.fold_in(arg_keys[7], 71), 0)
    w_uv = normal_values(arg_keys[3], (H, R, V), (R // 16) ** -0.5, 1.0, ((0, 4),))
    fork_prompt_keys = jax.random.split(jax.random.fold_in(arg_keys[4], 1), FORKS // FORK_DEV)
    fork_prompt_turns = jax.random.permutation(jax.random.fold_in(arg_keys[4], 3), FORKS // FORK_DEV)
    fork_prompt = jax.vmap(lambda own, number: shared_out(jax.random.fold_in(arg_keys[4], 2), own, number, FORK_DEV, PROMPTS, 1, MOST, 2))(fork_prompt_keys, fork_prompt_turns).reshape((FORKS, 1))
    prompt_slot = jax.random.permutation(arg_keys[5], PROMPTS).astype(jnp.int32)
    suffix_len = set_ends(jax.random.randint(arg_keys[6], (FORKS,), S // 4, S + 1), jax.random.fold_in(arg_keys[6], 1), S // 4, S).astype(jnp.int32)
    return {"queries": queries, "prefix_cache": prefix_cache, "suffix_cache": suffix_cache, "w_uv": w_uv, "fork_prompt": fork_prompt, "prompt_slot": prompt_slot, "suffix_len": suffix_len}


score_scale = 192.0 ** -0.5


def attend(query_heads, keys, live_mask):
    scores = jnp.einsum('bhe,bek->bhk', query_heads, keys) * score_scale
    scores = jnp.where(live_mask, scores, -jnp.inf)
    peak = jnp.max(scores, axis=2, keepdims=True)
    weights = jnp.where(live_mask, jnp.exp(scores - peak), 0.0)
    mass_sum = jnp.sum(weights, axis=2)
    rounded = lax.optimization_barrier(weights.astype(jnp.bfloat16)).astype(jnp.float32)
    summed = jnp.einsum('bhk,brk->bhr', rounded, keys[:, :R, :])
    latent = (summed / mass_sum[..., None]).astype(jnp.bfloat16)
    return latent, peak[..., 0] + jnp.log(mass_sum)


def project(latent, w_full):
    return jnp.einsum('bhr,hrv->bhv', latent.astype(jnp.float32), w_full).astype(jnp.bfloat16)


def reference(queries, prefix_cache, suffix_cache, w_uv, fork_prompt, prompt_slot, suffix_len):
    owner_slot = jnp.take(prompt_slot, fork_prompt[:, 0]).astype(jnp.int32)
    blocks = FORKS // FORK_DEV
    w_full = w_uv.astype(jnp.float32)

    def one_block(items):
        block_queries, block_suffix, block_owner, block_lengths = items
        query_heads = block_queries.astype(jnp.float32).reshape(FORK_DEV, H, R + P_SIZE)
        prefix_keys = jnp.take(prefix_cache, block_owner, axis=0).astype(jnp.float32)
        all_live = jnp.ones((FORK_DEV, 1, L), dtype=bool)
        latent_prefix, mass_prefix = attend(query_heads, prefix_keys, all_live)
        positions = jnp.arange(S).astype(jnp.int32)
        suffix_live = (positions[None, :] < block_lengths[:, None])[:, None, :]
        latent_suffix, mass_suffix = attend(query_heads, block_suffix.astype(jnp.float32), suffix_live)
        value_prefix = project(latent_prefix, w_full).astype(jnp.float32)
        value_suffix = project(latent_suffix, w_full).astype(jnp.float32)
        top_mass = jnp.maximum(mass_prefix, mass_suffix)
        share_prefix = jnp.exp(mass_prefix - top_mass)[..., None]
        share_suffix = jnp.exp(mass_suffix - top_mass)[..., None]
        combined = (share_prefix * value_prefix + share_suffix * value_suffix) / (share_prefix + share_suffix)
        return combined.astype(jnp.bfloat16).reshape(FORK_DEV, H * V)

    result = lax.map(one_block, (queries.reshape(blocks, FORK_DEV, H * (R + P_SIZE)),
                                 suffix_cache.reshape(blocks, FORK_DEV, R + P_SIZE, S),
                                 owner_slot.reshape(blocks, FORK_DEV),
                                 suffix_len.reshape(blocks, FORK_DEV)))
    return result.reshape(FORKS, H * V)
```

```python
import functools

import jax
import jax.numpy as jnp
from jax import lax
from jax.experimental import pallas as pl
from jax.experimental.pallas import tpu as pltpu
from jax.sharding import PartitionSpec as P

R = 512
P_SIZE = 64
V = 128


score_scale = 192.0 ** (-0.5)
log2e = 1.4426950408889634
OUTER = (((1,), (1,)), ((), ()))


def project(latent, w_uv):
    return jnp.einsum("nhr,hrv->nhv", latent, w_uv, preferred_element_type=jnp.float32).astype(
        jnp.bfloat16
    )


def exchange_plan(queries, prefix_cache, suffix_cache, w_uv, fork_prompt, prompt_slot, suffix_len):
    owners_count = lax.axis_size("dp")
    forks_here = queries.shape[0]
    heads_here = w_uv.shape[0]
    key_width = R + P_SIZE
    capacity = max(2, 2 * forks_here // owners_count)
    slots_all = owners_count * capacity
    prompt_ids = jnp.arange(prompt_slot.shape[0], dtype=jnp.int32)
    chosen = fork_prompt[:, 0][:, None] == prompt_ids[None, :]
    owner_slot = jnp.sum(jnp.where(chosen, prompt_slot[None, :], 0), axis=1)
    fork_order = jnp.arange(forks_here, dtype=jnp.int32)
    before = (owner_slot[:, None] == owner_slot[None, :]) & (
        fork_order[None, :] < fork_order[:, None]
    )
    slot_rank = jnp.sum(before.astype(jnp.int32), axis=1)
    target = owner_slot * capacity + slot_rank
    placing = target[None, :] == jnp.arange(slots_all, dtype=jnp.int32)[:, None]
    outbound = jnp.dot(
        placing.astype(jnp.bfloat16), queries, preferred_element_type=jnp.float32
    ).astype(jnp.bfloat16)
    outbound = outbound.reshape(owners_count, capacity, heads_here * key_width)
    gathered = lax.all_gather(prefix_cache, "tp", axis=2, tiled=True)[0]
    received = lax.all_to_all(outbound, "dp", split_axis=0, concat_axis=0, tiled=True)
    sources = received.shape[0]
    items = received.shape[1]
    lead_rows = sources * items
    query_rows = received.reshape(lead_rows * heads_here, key_width)
    scores = jnp.dot(query_rows, gathered, preferred_element_type=jnp.float32) * score_scale
    peak_score = jnp.max(scores, axis=1, keepdims=True)
    weights = jnp.exp(scores - peak_score)
    mass_sum = jnp.sum(weights, axis=1)
    summed = lax.dot_general(
        weights.astype(jnp.bfloat16),
        gathered[:R],
        (((1,), (1,)), ((), ())),
        preferred_element_type=jnp.float32,
    )
    latent = (summed / mass_sum[:, None]).astype(jnp.bfloat16)
    log_mass = (peak_score[:, 0] + jnp.log(mass_sum)).reshape(sources, items, heads_here)
    result = project(latent.reshape(lead_rows, heads_here, R), w_uv)
    result = result.reshape(sources, items, heads_here * V)
    answer, answer_mass = (
        lax.all_to_all(result, "dp", split_axis=0, concat_axis=0, tiled=True),
        lax.all_to_all(
            log_mass.astype(jnp.bfloat16), "dp", split_axis=0, concat_axis=0, tiled=True
        ).astype(log_mass.dtype),
    )
    picking = placing.astype(jnp.bfloat16)
    flat_answer = answer.reshape(slots_all, answer.shape[2])
    returned = lax.dot_general(
        picking, flat_answer, (((0,), (0,)), ((), ())), preferred_element_type=jnp.float32
    ).astype(jnp.bfloat16)
    mass_prefix = lax.dot_general(
        placing.astype(jnp.float32),
        answer_mass.reshape(slots_all, heads_here),
        (((0,), (0,)), ((), ())),
        precision=lax.Precision.HIGHEST,
    )
    value_prefix = returned.reshape(forks_here, heads_here, V)
    query_heads = queries.reshape(forks_here, heads_here, key_width)
    suffix_scores = (
        jnp.einsum("fhe,fes->fhs", query_heads, suffix_cache, preferred_element_type=jnp.float32)
        * score_scale
    )
    positions = jnp.arange(suffix_cache.shape[2], dtype=jnp.int32)
    live_mask = (positions[None, :] < suffix_len[:, None])[:, None, :]
    suffix_scores = jnp.where(live_mask, suffix_scores, -jnp.inf)
    suffix_peak = jnp.max(suffix_scores, axis=2, keepdims=True)
    suffix_weights = jnp.where(live_mask, jnp.exp(suffix_scores - suffix_peak), 0.0)
    suffix_sum = jnp.sum(suffix_weights, axis=2)
    suffix_summed = jnp.einsum(
        "fhs,frs->fhr",
        suffix_weights.astype(jnp.bfloat16),
        suffix_cache[:, :R, :],
        preferred_element_type=jnp.float32,
    )
    latent_suffix = (suffix_summed / suffix_sum[..., None]).astype(jnp.bfloat16)
    mass_suffix = suffix_peak[..., 0] + jnp.log(suffix_sum)
    value_suffix = project(latent_suffix, w_uv)
    top_mass = jnp.maximum(mass_prefix, mass_suffix)
    share_prefix = jnp.exp(mass_prefix - top_mass)[..., None]
    share_suffix = jnp.exp(mass_suffix - top_mass)[..., None]
    combined = (
        share_prefix * value_prefix.astype(jnp.float32)
        + share_suffix * value_suffix.astype(jnp.float32)
    ) / (share_prefix + share_suffix)
    return combined.astype(jnp.bfloat16).reshape(forks_here, heads_here * V)


def suffix_kernel(lens_ref, q_ref, cache_ref, latent_ref, mass_ref):
    block = q_ref.shape[0]
    first = pl.program_id(0) * block
    positions = lax.broadcasted_iota(jnp.int32, (1, cache_ref.shape[2]), 1)
    for i in range(block):
        live = positions < lens_ref[first + i]
        scores = jnp.dot(q_ref[i], cache_ref[i], preferred_element_type=jnp.float32)
        scores = jnp.where(live, scores * score_scale, -jnp.inf)
        peak = jnp.max(scores, axis=1, keepdims=True)
        weights = jnp.exp(scores - peak)
        mass = jnp.sum(weights, axis=1, keepdims=True)
        summed = lax.dot_general(
            weights.astype(jnp.bfloat16),
            cache_ref[i, :R, :],
            OUTER,
            preferred_element_type=jnp.float32,
        )
        latent_ref[i] = (summed / mass).astype(jnp.bfloat16)
        mass_ref[i] = jnp.broadcast_to(peak + jnp.log(mass), mass_ref.shape[1:])


def suffix_attention(query_heads, suffix_cache, suffix_len, block=8):
    forks, heads, width = query_heads.shape
    keys = suffix_cache.shape[2]
    return pl.pallas_call(
        suffix_kernel,
        grid_spec=pltpu.PrefetchScalarGridSpec(
            num_scalar_prefetch=1,
            grid=(forks // block,),
            in_specs=[
                pl.BlockSpec((block, heads, width), lambda i, lens: (i, 0, 0)),
                pl.BlockSpec((block, width, keys), lambda i, lens: (i, 0, 0)),
            ],
            out_specs=[
                pl.BlockSpec((block, heads, R), lambda i, lens: (i, 0, 0)),
                pl.BlockSpec((block, heads, 128), lambda i, lens: (i, 0, 0)),
            ],
        ),
        out_shape=[
            jax.ShapeDtypeStruct((forks, heads, R), jnp.bfloat16),
            jax.ShapeDtypeStruct((forks, heads, 128), jnp.float32),
        ],
        cost_estimate=pl.CostEstimate(
            flops=16 * forks * heads * keys * (width + R),
            bytes_accessed=2 * suffix_cache.size + 2 * query_heads.size,
            transcendentals=forks * heads * keys,
        ),
        name="suffix",
    )(suffix_len, query_heads, suffix_cache)


def prefix_kernel(
    group, starts_ref, order_ref, q_ref, cache_ref, latent_ref, mass_ref, out_ref
):
    slot = pl.program_id(0)
    heads = q_ref.shape[1]
    first = starts_ref[slot]
    last = starts_ref[slot + 1] - 1
    parts = cache_ref.shape[1]

    def one_group(g, carry):
        ids = [order_ref[jnp.minimum(first + g * group + i, last)] for i in range(group)]
        rows = jnp.concatenate([q_ref[fork] for fork in ids], axis=0)
        scores = [
            jnp.dot(rows, cache_ref[0, k], preferred_element_type=jnp.float32)
            for k in range(parts)
        ]
        peak = functools.reduce(
            jnp.maximum, [jnp.max(piece, axis=1, keepdims=True) for piece in scores]
        )
        mass = 0.0
        summed = 0.0
        for k in range(parts):
            weights = jnp.exp2((scores[k] - peak) * (score_scale * log2e))
            mass = mass + jnp.sum(weights, axis=1, keepdims=True)
            summed = summed + lax.dot_general(
                weights.astype(jnp.bfloat16),
                cache_ref[0, k, :R, :],
                OUTER,
                preferred_element_type=jnp.float32,
            )
        peak = peak * score_scale
        for i, fork in enumerate(ids):
            own = slice(i * heads, (i + 1) * heads)
            other = mass_ref[fork][:, :1]
            top = jnp.maximum(peak[own], other)
            ours = jnp.exp(peak[own] - top)
            theirs = jnp.exp(other - top)
            share = 1.0 / (ours * mass[own] + theirs)
            out_ref[fork] = (
                summed[own] * (ours * share)
                + latent_ref[fork].astype(jnp.float32) * (theirs * share)
            ).astype(jnp.bfloat16)
        return carry

    lax.fori_loop(0, (last - first + group) // group, one_group, 0)


def prefix_attention(starts, order, query_heads, caches, latent_suffix, mass_suffix, group=8):
    forks, heads, width = query_heads.shape
    slots, parts, _, keys = caches.shape
    whole = lambda s, a, b: (0, 0, 0)
    return pl.pallas_call(
        functools.partial(prefix_kernel, group),
        grid_spec=pltpu.PrefetchScalarGridSpec(
            num_scalar_prefetch=2,
            grid=(slots,),
            in_specs=[
                pl.BlockSpec((forks, heads, width), whole),
                pl.BlockSpec((1, parts, width, keys), lambda s, a, b: (s, 0, 0, 0)),
                pl.BlockSpec((forks, heads, R), whole),
                pl.BlockSpec((forks, heads, 128), whole),
            ],
            out_specs=pl.BlockSpec((forks, heads, R), whole),
        ),
        out_shape=jax.ShapeDtypeStruct((forks, heads, R), jnp.bfloat16),
        cost_estimate=pl.CostEstimate(
            flops=2 * forks * heads * parts * keys * (width + R),
            bytes_accessed=2 * caches.size + 2 * query_heads.size,
            transcendentals=forks * heads * parts * keys,
        ),
        compiler_params=pltpu.CompilerParams(vmem_limit_bytes=48 * 1024 * 1024),
        name="prefix",
    )(starts, order, query_heads, caches, latent_suffix, mass_suffix)


def fork_order(fork_prompt, prompt_slot):
    forks = fork_prompt.shape[0]
    prompt_ids = jnp.arange(prompt_slot.shape[0], dtype=jnp.int32)
    chosen = fork_prompt[:, 0][:, None] == prompt_ids[None, :]
    owner_slot = jnp.sum(jnp.where(chosen, prompt_slot[None, :], 0), axis=1)
    ids = jnp.arange(forks, dtype=jnp.int32)
    key = owner_slot * forks + ids
    place = jnp.sum((key[None, :] < key[:, None]).astype(jnp.int32), axis=1)
    order = jnp.sum(jnp.where(place[None, :] == ids[:, None], ids[None, :], 0), axis=1)
    edges = jnp.arange(prompt_slot.shape[0] + 1, dtype=jnp.int32)
    starts = jnp.sum((owner_slot[None, :] < edges[:, None]).astype(jnp.int32), axis=1)
    return starts, order


def gather_plan(queries, prefix_cache, suffix_cache, w_uv, fork_prompt, prompt_slot, suffix_len):
    forks_here = queries.shape[0]
    heads_here = w_uv.shape[0]
    owners_count = lax.axis_size("dp")
    tp_count = lax.axis_size("tp")
    caches = lax.all_gather(prefix_cache[0], ("dp", "tp"), axis=0)
    caches = caches.reshape(owners_count, tp_count, *prefix_cache.shape[1:])
    starts, order = fork_order(fork_prompt, prompt_slot)
    query_heads = queries.reshape(forks_here, heads_here, R + P_SIZE)
    latent_suffix, mass_suffix = suffix_attention(query_heads, suffix_cache, suffix_len)
    latent = prefix_attention(starts, order, query_heads, caches, latent_suffix, mass_suffix)
    return project(latent, w_uv).reshape(forks_here, heads_here * V)


def shards(queries, prefix_cache, *others):
    owners_count = lax.axis_size("dp")
    forks_here = queries.shape[0]
    capacity = max(2, 2 * forks_here // owners_count)
    sent = owners_count * capacity * queries.shape[1]
    gathered = owners_count * lax.axis_size("tp") * prefix_cache.size
    plan = gather_plan if gathered <= 4 * sent else exchange_plan
    return plan(queries, prefix_cache, *others)


def solution(mesh):
    placed = (
        P("dp", "tp"),
        P("dp", None, "tp"),
        P("dp", None, None),
        P("tp", None, None),
        P("dp", None),
        P(),
        P("dp"),
    )
    return jax.shard_map(
        shards, mesh=mesh, in_specs=placed, out_specs=P("dp", "tp"), check_vma=False
    )
```

```python
import functools

import jax
import jax.numpy as jnp
from jax import lax
from jax.experimental import pallas as pl
from jax.experimental.pallas import tpu as pltpu
from jax.sharding import PartitionSpec as P

R = 512
P_SIZE = 64
V = 128


score_scale = 192.0 ** (-0.5)
log2e = 1.4426950408889634
OUTER = (((1,), (1,)), ((), ()))


def project(latent, w_uv):
    return jnp.einsum("nhr,hrv->nhv", latent, w_uv, preferred_element_type=jnp.float32).astype(
        jnp.bfloat16
    )


def exchange_plan(queries, prefix_cache, suffix_cache, w_uv, fork_prompt, prompt_slot, suffix_len):
    owners_count = lax.axis_size("dp")
    forks_here = queries.shape[0]
    heads_here = w_uv.shape[0]
    key_width = R + P_SIZE
    capacity = max(2, 2 * forks_here // owners_count)
    slots_all = owners_count * capacity
    prompt_ids = jnp.arange(prompt_slot.shape[0], dtype=jnp.int32)
    chosen = fork_prompt[:, 0][:, None] == prompt_ids[None, :]
    owner_slot = jnp.sum(jnp.where(chosen, prompt_slot[None, :], 0), axis=1)
    fork_order = jnp.arange(forks_here, dtype=jnp.int32)
    before = (owner_slot[:, None] == owner_slot[None, :]) & (
        fork_order[None, :] < fork_order[:, None]
    )
    slot_rank = jnp.sum(before.astype(jnp.int32), axis=1)
    target = owner_slot * capacity + slot_rank
    placing = target[None, :] == jnp.arange(slots_all, dtype=jnp.int32)[:, None]
    outbound = jnp.dot(
        placing.astype(jnp.bfloat16), queries, preferred_element_type=jnp.float32
    ).astype(jnp.bfloat16)
    outbound = outbound.reshape(owners_count, capacity, heads_here * key_width)
    gathered = lax.all_gather(prefix_cache, "tp", axis=2, tiled=True)[0]
    received = lax.all_to_all(outbound, "dp", split_axis=0, concat_axis=0, tiled=True)
    sources = received.shape[0]
    items = received.shape[1]
    lead_rows = sources * items
    query_rows = received.reshape(lead_rows * heads_here, key_width)
    scores = jnp.dot(query_rows, gathered, preferred_element_type=jnp.float32) * score_scale
    peak_score = jnp.max(scores, axis=1, keepdims=True)
    weights = jnp.exp(scores - peak_score)
    mass_sum = jnp.sum(weights, axis=1)
    summed = lax.dot_general(
        weights.astype(jnp.bfloat16),
        gathered[:R],
        (((1,), (1,)), ((), ())),
        preferred_element_type=jnp.float32,
    )
    latent = (summed / mass_sum[:, None]).astype(jnp.bfloat16)
    log_mass = (peak_score[:, 0] + jnp.log(mass_sum)).reshape(sources, items, heads_here)
    result = project(latent.reshape(lead_rows, heads_here, R), w_uv)
    result = result.reshape(sources, items, heads_here * V)
    answer, answer_mass = (
        lax.all_to_all(result, "dp", split_axis=0, concat_axis=0, tiled=True),
        lax.all_to_all(
            log_mass.astype(jnp.bfloat16), "dp", split_axis=0, concat_axis=0, tiled=True
        ).astype(log_mass.dtype),
    )
    picking = placing.astype(jnp.bfloat16)
    flat_answer = answer.reshape(slots_all, answer.shape[2])
    returned = lax.dot_general(
        picking, flat_answer, (((0,), (0,)), ((), ())), preferred_element_type=jnp.float32
    ).astype(jnp.bfloat16)
    mass_prefix = lax.dot_general(
        placing.astype(jnp.float32),
        answer_mass.reshape(slots_all, heads_here),
        (((0,), (0,)), ((), ())),
        precision=lax.Precision.HIGHEST,
    )
    value_prefix = returned.reshape(forks_here, heads_here, V)
    query_heads = queries.reshape(forks_here, heads_here, key_width)
    suffix_scores = (
        jnp.einsum("fhe,fes->fhs", query_heads, suffix_cache, preferred_element_type=jnp.float32)
        * score_scale
    )
    positions = jnp.arange(suffix_cache.shape[2], dtype=jnp.int32)
    live_mask = (positions[None, :] < suffix_len[:, None])[:, None, :]
    suffix_scores = jnp.where(live_mask, suffix_scores, -jnp.inf)
    suffix_peak = jnp.max(suffix_scores, axis=2, keepdims=True)
    suffix_weights = jnp.where(live_mask, jnp.exp(suffix_scores - suffix_peak), 0.0)
    suffix_sum = jnp.sum(suffix_weights, axis=2)
    suffix_summed = jnp.einsum(
        "fhs,frs->fhr",
        suffix_weights.astype(jnp.bfloat16),
        suffix_cache[:, :R, :],
        preferred_element_type=jnp.float32,
    )
    latent_suffix = (suffix_summed / suffix_sum[..., None]).astype(jnp.bfloat16)
    mass_suffix = suffix_peak[..., 0] + jnp.log(suffix_sum)
    value_suffix = project(latent_suffix, w_uv)
    top_mass = jnp.maximum(mass_prefix, mass_suffix)
    share_prefix = jnp.exp(mass_prefix - top_mass)[..., None]
    share_suffix = jnp.exp(mass_suffix - top_mass)[..., None]
    combined = (
        share_prefix * value_prefix.astype(jnp.float32)
        + share_suffix * value_suffix.astype(jnp.float32)
    ) / (share_prefix + share_suffix)
    return combined.astype(jnp.bfloat16).reshape(forks_here, heads_here * V)


MESH = pl.DeviceIdType.MESH


def suffix_fork(i, lens_ref, q_ref, cache_ref, latent_ref, mass_ref):
    positions = lax.broadcasted_iota(jnp.int32, (1, cache_ref.shape[2]), 1)
    live = positions < lens_ref[i]
    scores = jnp.dot(q_ref[i], cache_ref[i], preferred_element_type=jnp.float32)
    scores = jnp.where(live, scores * score_scale, -jnp.inf)
    peak = jnp.max(scores, axis=1, keepdims=True)
    weights = jnp.exp(scores - peak)
    mass = jnp.sum(weights, axis=1, keepdims=True)
    summed = lax.dot_general(
        weights.astype(jnp.bfloat16),
        cache_ref[i, :R, :],
        OUTER,
        preferred_element_type=jnp.float32,
    )
    latent_ref[i] = (summed / mass).astype(jnp.bfloat16)
    mass_ref[i] = jnp.broadcast_to(peak + jnp.log(mass), mass_ref.shape[1:])


def gather_kernel(
    planes,
    steps,
    lens_ref,
    own_ref,
    q_ref,
    suffix_ref,
    out_ref,
    latent_ref,
    mass_ref,
    held,
    load_sem,
    own_sem,
    z_send,
    z_recv,
    x_send,
    x_recv,
    y_send,
    y_recv,
    dx_send,
    dx_recv,
    dy_send,
    dy_recv,
    pair_send,
    pair_recv,
):
    dp, tp = lax.axis_index("dp"), lax.axis_index("tp")
    z, x = dp // 2, dp % 2
    y, c = tp // 2, tp % 2
    forks = q_ref.shape[0]
    block = forks // steps
    half = own_ref.shape[1] // 2
    at_x = (z * 2 + (1 - x), tp)
    at_y = (dp, (1 - y) * 2 + c)
    at_pair = (dp, y * 2 + (1 - c))
    at_up = (jnp.minimum(z + 1, planes - 1) * 2 + x, tp)
    at_down = (jnp.maximum(z - 1, 0) * 2 + x, tp)
    has_up, has_down = z + 1 < planes, z > 0

    def place(zz, xx, yy):
        return out_ref.at[zz * 2 + xx, yy * 2 + c]

    def top(ref):
        return ref.at[pl.ds(0, half)]

    def bottom(ref):
        return ref.at[pl.ds(half, half)]

    def copy(src, dst, send, recv, device):
        return pltpu.make_async_remote_copy(
            src_ref=src,
            dst_ref=dst,
            send_sem=send,
            recv_sem=recv,
            device_id=device,
            device_id_type=MESH,
        )

    def z_copy(zz, device, src=None):
        to = place(zz, x, y)
        return copy(to if src is None else src, to, z_send.at[zz], z_recv.at[zz], device)

    def own_up(device, src):
        to = place(z, x, y)
        return copy(src, to, z_send.at[planes], z_recv.at[z], device)

    def x_copy(zz, src=None):
        to = place(zz, x, y)
        return copy(to if src is None else src, to, x_send.at[zz], x_recv.at[zz], at_x)

    def y_copy(zz, src=None):
        to = place(zz, x, y)
        return copy(to if src is None else src, to, y_send.at[zz], y_recv.at[zz], at_y)

    def dy_copy(zz):
        part = top(place(zz, 1 - x, y))
        return copy(part, part, dy_send.at[zz], dy_recv.at[zz], at_y)

    def dx_copy(zz):
        part = bottom(place(zz, x, 1 - y))
        return copy(part, part, dx_send.at[zz], dx_recv.at[zz], at_x)

    def pair_copy(zz, xx, yy, src=None):
        to = place(zz, xx, yy)
        k = (zz * 2 + xx) * 2 + yy
        src = to if src is None else src
        return copy(src, to, pair_send.at[k], pair_recv.at[k], at_pair)

    def load(s):
        part = pl.ds(s * block, block)
        return pltpu.make_async_copy(suffix_ref.at[part], held.at[part], load_sem.at[s])

    for s in range(steps):
        load(s).start()

    barrier = pltpu.get_barrier_semaphore()
    for device in (at_x, at_y, at_pair):
        pl.semaphore_signal(barrier, inc=1, device_id=device, device_id_type=MESH)

    @pl.when(has_up)
    def _():
        pl.semaphore_signal(barrier, inc=1, device_id=at_up, device_id_type=MESH)

    @pl.when(has_down)
    def _():
        pl.semaphore_signal(barrier, inc=1, device_id=at_down, device_id_type=MESH)

    pl.semaphore_wait(barrier, 3 + has_up.astype(jnp.int32) + has_down.astype(jnp.int32))

    mine = own_ref.at[0]

    @pl.when(has_up)
    def _():
        z_copy(z, at_up, mine).start()

    @pl.when(has_down)
    def _():
        own_up(at_down, mine).start()

    x_copy(z, mine).start()
    y_copy(z, mine).start()
    pair_copy(z, x, y, mine).start()
    local = pltpu.make_async_copy(mine, place(z, x, y), own_sem)
    local.start()

    def compute(low, high):
        def step(s, carry):
            load(s).wait()
            for i in range(block):
                suffix_fork(s * block + i, lens_ref, q_ref, held, latent_ref, mass_ref)
            return carry

        lax.fori_loop(low, high, step, 0)

    def arrived(d):
        for sign in (-1, 1):
            zz = z + sign * d
            onward = has_up if sign < 0 else has_down
            device = at_up if sign < 0 else at_down

            @pl.when((zz >= 0) & (zz < planes))
            def _():
                z_copy(zz, device).wait_recv()

                @pl.when(onward)
                def _():
                    z_copy(zz, device).start()

                x_copy(zz).start()
                y_copy(zz).start()
                pair_copy(zz, x, y).start()

    def each(d, act):
        if d == 0:
            act(z)
            return
        for sign in (-1, 1):
            zz = z + sign * d
            pl.when((zz >= 0) & (zz < planes))(functools.partial(act, zz))

    def across(zz):
        x_copy(zz).wait_recv()
        dy_copy(zz).start()
        pair_copy(zz, 1 - x, y).start()
        y_copy(zz).wait_recv()
        dx_copy(zz).start()
        pair_copy(zz, x, 1 - y).start()

    def diagonal(zz):
        dy_copy(zz).wait_recv()
        dx_copy(zz).wait_recv()
        pair_copy(zz, 1 - x, 1 - y).start()

    marks = [steps * r // planes for r in range(planes + 1)]
    for r in range(planes):
        if r > 0:
            arrived(r)
            each(r - 1, across)
        if r > 1:
            each(r - 2, diagonal)
        compute(marks[r], marks[r + 1])
    each(planes - 1, across)
    if planes > 1:
        each(planes - 2, diagonal)
    each(planes - 1, diagonal)

    local.wait()

    @pl.when(has_down)
    def _():
        own_up(at_down, mine).wait_send()

    for zz in range(planes):
        sent = ((zz <= z) & has_up) | ((zz > z) & has_down)

        @pl.when(sent)
        def _():
            z_copy(zz, at_up).wait_send()

        x_copy(zz).wait_send()
        y_copy(zz).wait_send()
        dx_copy(zz).wait_send()
        dy_copy(zz).wait_send()
        for xx in range(2):
            for yy in range(2):
                pair_copy(zz, xx, yy).wait()


def gather_and_suffix(prefix_cache, query_heads, suffix_cache, suffix_len, steps=8):
    forks, heads, width = query_heads.shape
    keys = suffix_cache.shape[2]
    slots, parts = lax.axis_size("dp"), lax.axis_size("tp")
    planes = slots // 2
    dma = pltpu.SemaphoreType.DMA
    vmem = pl.BlockSpec(memory_space=pltpu.VMEM)
    hbm = pl.BlockSpec(memory_space=pl.ANY)
    return pl.pallas_call(
        functools.partial(gather_kernel, planes, steps),
        in_specs=[pl.BlockSpec(memory_space=pltpu.SMEM), hbm, vmem, hbm],
        out_specs=[hbm, vmem, vmem],
        out_shape=[
            jax.ShapeDtypeStruct((slots, parts, *prefix_cache.shape[1:]), jnp.bfloat16),
            jax.ShapeDtypeStruct((forks, heads, R), jnp.bfloat16),
            jax.ShapeDtypeStruct((forks, heads, 128), jnp.float32),
        ],
        scratch_shapes=[
            pltpu.VMEM(suffix_cache.shape, jnp.bfloat16),
            dma((steps,)),
            dma,
            dma((planes + 1,)),
            *[dma((planes,)) for _ in range(9)],
            dma((slots * 2,)),
            dma((slots * 2,)),
        ],
        compiler_params=pltpu.CompilerParams(
            collective_id=0, has_side_effects=True, vmem_limit_bytes=40 * 1024 * 1024
        ),
        name="gather",
    )(suffix_len, prefix_cache, query_heads, suffix_cache)


def prefix_kernel(
    group, starts_ref, order_ref, q_ref, cache_ref, latent_ref, mass_ref, out_ref
):
    slot = pl.program_id(0)
    heads = q_ref.shape[1]
    first = starts_ref[slot]
    last = starts_ref[slot + 1] - 1
    parts = cache_ref.shape[1]

    def one_group(g, carry):
        ids = [order_ref[jnp.minimum(first + g * group + i, last)] for i in range(group)]
        rows = jnp.concatenate([q_ref[fork] for fork in ids], axis=0)
        scores = [
            jnp.dot(rows, cache_ref[0, k], preferred_element_type=jnp.float32)
            for k in range(parts)
        ]
        peak = functools.reduce(
            jnp.maximum, [jnp.max(piece, axis=1, keepdims=True) for piece in scores]
        )
        mass = 0.0
        summed = 0.0
        for k in range(parts):
            weights = jnp.exp2((scores[k] - peak) * (score_scale * log2e))
            mass = mass + jnp.sum(weights, axis=1, keepdims=True)
            summed = summed + lax.dot_general(
                weights.astype(jnp.bfloat16),
                cache_ref[0, k, :R, :],
                OUTER,
                preferred_element_type=jnp.float32,
            )
        peak = peak * score_scale
        for i, fork in enumerate(ids):
            own = slice(i * heads, (i + 1) * heads)
            other = mass_ref[fork][:, :1]
            top = jnp.maximum(peak[own], other)
            ours = jnp.exp(peak[own] - top)
            theirs = jnp.exp(other - top)
            share = 1.0 / (ours * mass[own] + theirs)
            out_ref[fork] = (
                summed[own] * (ours * share)
                + latent_ref[fork].astype(jnp.float32) * (theirs * share)
            ).astype(jnp.bfloat16)
        return carry

    lax.fori_loop(0, (last - first + group) // group, one_group, 0)


def prefix_attention(starts, order, query_heads, caches, latent_suffix, mass_suffix, group=8):
    forks, heads, width = query_heads.shape
    slots, parts, _, keys = caches.shape
    whole = lambda s, a, b: (0, 0, 0)
    return pl.pallas_call(
        functools.partial(prefix_kernel, group),
        grid_spec=pltpu.PrefetchScalarGridSpec(
            num_scalar_prefetch=2,
            grid=(slots,),
            in_specs=[
                pl.BlockSpec((forks, heads, width), whole),
                pl.BlockSpec((1, parts, width, keys), lambda s, a, b: (s, 0, 0, 0)),
                pl.BlockSpec((forks, heads, R), whole),
                pl.BlockSpec((forks, heads, 128), whole),
            ],
            out_specs=pl.BlockSpec((forks, heads, R), whole),
        ),
        out_shape=jax.ShapeDtypeStruct((forks, heads, R), jnp.bfloat16),
        cost_estimate=pl.CostEstimate(
            flops=2 * forks * heads * parts * keys * (width + R),
            bytes_accessed=2 * caches.size + 2 * query_heads.size,
            transcendentals=forks * heads * parts * keys,
        ),
        compiler_params=pltpu.CompilerParams(vmem_limit_bytes=48 * 1024 * 1024),
        name="prefix",
    )(starts, order, query_heads, caches, latent_suffix, mass_suffix)


def fork_order(fork_prompt, prompt_slot):
    forks = fork_prompt.shape[0]
    prompt_ids = jnp.arange(prompt_slot.shape[0], dtype=jnp.int32)
    chosen = fork_prompt[:, 0][:, None] == prompt_ids[None, :]
    owner_slot = jnp.sum(jnp.where(chosen, prompt_slot[None, :], 0), axis=1)
    ids = jnp.arange(forks, dtype=jnp.int32)
    key = owner_slot * forks + ids
    place = jnp.sum((key[None, :] < key[:, None]).astype(jnp.int32), axis=1)
    order = jnp.sum(jnp.where(place[None, :] == ids[:, None], ids[None, :], 0), axis=1)
    edges = jnp.arange(prompt_slot.shape[0] + 1, dtype=jnp.int32)
    starts = jnp.sum((owner_slot[None, :] < edges[:, None]).astype(jnp.int32), axis=1)
    return starts, order


def gather_plan(queries, prefix_cache, suffix_cache, w_uv, fork_prompt, prompt_slot, suffix_len):
    forks_here = queries.shape[0]
    heads_here = w_uv.shape[0]
    starts, order = fork_order(fork_prompt, prompt_slot)
    query_heads = queries.reshape(forks_here, heads_here, R + P_SIZE)
    caches, latent_suffix, mass_suffix = gather_and_suffix(
        prefix_cache, query_heads, suffix_cache, suffix_len
    )
    latent = prefix_attention(starts, order, query_heads, caches, latent_suffix, mass_suffix)
    return project(latent, w_uv).reshape(forks_here, heads_here * V)


def shards(queries, prefix_cache, *others):
    owners_count = lax.axis_size("dp")
    forks_here = queries.shape[0]
    capacity = max(2, 2 * forks_here // owners_count)
    sent = owners_count * capacity * queries.shape[1]
    gathered = owners_count * lax.axis_size("tp") * prefix_cache.size
    square = lax.axis_size("tp") == 4 and owners_count % 2 == 0
    plan = gather_plan if square and gathered <= 4 * sent else exchange_plan
    return plan(queries, prefix_cache, *others)


def solution(mesh):
    placed = (
        P("dp", "tp"),
        P("dp", None, "tp"),
        P("dp", None, None),
        P("tp", None, None),
        P("dp", None),
        P(),
        P("dp"),
    )
    return jax.shard_map(
        shards, mesh=mesh, in_specs=placed, out_specs=P("dp", "tp"), check_vma=False
    )
```

```python
import functools
import math

import jax
import jax.numpy as jnp
from jax import lax
from jax.experimental import pallas as pl
from jax.experimental.pallas import tpu as pltpu
from jax.sharding import PartitionSpec as P

R = 512
P_SIZE = 64
V = 128


score_scale = 192.0 ** (-0.5)
log2e = 1.4426950408889634
OUTER = (((1,), (1,)), ((), ()))


def project(latent, w_uv):
    return jnp.einsum("nhr,hrv->nhv", latent, w_uv, preferred_element_type=jnp.float32).astype(
        jnp.bfloat16
    )


def exchange_plan(queries, prefix_cache, suffix_cache, w_uv, fork_prompt, prompt_slot, suffix_len):
    owners_count = lax.axis_size("dp")
    forks_here = queries.shape[0]
    heads_here = w_uv.shape[0]
    key_width = R + P_SIZE
    capacity = max(2, 2 * forks_here // owners_count)
    slots_all = owners_count * capacity
    prompt_ids = jnp.arange(prompt_slot.shape[0], dtype=jnp.int32)
    chosen = fork_prompt[:, 0][:, None] == prompt_ids[None, :]
    owner_slot = jnp.sum(jnp.where(chosen, prompt_slot[None, :], 0), axis=1)
    fork_order = jnp.arange(forks_here, dtype=jnp.int32)
    before = (owner_slot[:, None] == owner_slot[None, :]) & (
        fork_order[None, :] < fork_order[:, None]
    )
    slot_rank = jnp.sum(before.astype(jnp.int32), axis=1)
    target = owner_slot * capacity + slot_rank
    placing = target[None, :] == jnp.arange(slots_all, dtype=jnp.int32)[:, None]
    outbound = jnp.dot(
        placing.astype(jnp.bfloat16), queries, preferred_element_type=jnp.float32
    ).astype(jnp.bfloat16)
    outbound = outbound.reshape(owners_count, capacity, heads_here * key_width)
    gathered = lax.all_gather(prefix_cache, "tp", axis=2, tiled=True)[0]
    received = lax.all_to_all(outbound, "dp", split_axis=0, concat_axis=0, tiled=True)
    sources = received.shape[0]
    items = received.shape[1]
    lead_rows = sources * items
    query_rows = received.reshape(lead_rows * heads_here, key_width)
    scores = jnp.dot(query_rows, gathered, preferred_element_type=jnp.float32) * score_scale
    peak_score = jnp.max(scores, axis=1, keepdims=True)
    weights = jnp.exp(scores - peak_score)
    mass_sum = jnp.sum(weights, axis=1)
    summed = lax.dot_general(
        weights.astype(jnp.bfloat16),
        gathered[:R],
        (((1,), (1,)), ((), ())),
        preferred_element_type=jnp.float32,
    )
    latent = (summed / mass_sum[:, None]).astype(jnp.bfloat16)
    log_mass = (peak_score[:, 0] + jnp.log(mass_sum)).reshape(sources, items, heads_here)
    result = project(latent.reshape(lead_rows, heads_here, R), w_uv)
    result = result.reshape(sources, items, heads_here * V)
    answer, answer_mass = (
        lax.all_to_all(result, "dp", split_axis=0, concat_axis=0, tiled=True),
        lax.all_to_all(
            log_mass.astype(jnp.bfloat16), "dp", split_axis=0, concat_axis=0, tiled=True
        ).astype(log_mass.dtype),
    )
    picking = placing.astype(jnp.bfloat16)
    flat_answer = answer.reshape(slots_all, answer.shape[2])
    returned = lax.dot_general(
        picking, flat_answer, (((0,), (0,)), ((), ())), preferred_element_type=jnp.float32
    ).astype(jnp.bfloat16)
    mass_prefix = lax.dot_general(
        placing.astype(jnp.float32),
        answer_mass.reshape(slots_all, heads_here),
        (((0,), (0,)), ((), ())),
        precision=lax.Precision.HIGHEST,
    )
    value_prefix = returned.reshape(forks_here, heads_here, V)
    query_heads = queries.reshape(forks_here, heads_here, key_width)
    suffix_scores = (
        jnp.einsum("fhe,fes->fhs", query_heads, suffix_cache, preferred_element_type=jnp.float32)
        * score_scale
    )
    positions = jnp.arange(suffix_cache.shape[2], dtype=jnp.int32)
    live_mask = (positions[None, :] < suffix_len[:, None])[:, None, :]
    suffix_scores = jnp.where(live_mask, suffix_scores, -jnp.inf)
    suffix_peak = jnp.max(suffix_scores, axis=2, keepdims=True)
    suffix_weights = jnp.where(live_mask, jnp.exp(suffix_scores - suffix_peak), 0.0)
    suffix_sum = jnp.sum(suffix_weights, axis=2)
    suffix_summed = jnp.einsum(
        "fhs,frs->fhr",
        suffix_weights.astype(jnp.bfloat16),
        suffix_cache[:, :R, :],
        preferred_element_type=jnp.float32,
    )
    latent_suffix = (suffix_summed / suffix_sum[..., None]).astype(jnp.bfloat16)
    mass_suffix = suffix_peak[..., 0] + jnp.log(suffix_sum)
    value_suffix = project(latent_suffix, w_uv)
    top_mass = jnp.maximum(mass_prefix, mass_suffix)
    share_prefix = jnp.exp(mass_prefix - top_mass)[..., None]
    share_suffix = jnp.exp(mass_suffix - top_mass)[..., None]
    combined = (
        share_prefix * value_prefix.astype(jnp.float32)
        + share_suffix * value_suffix.astype(jnp.float32)
    ) / (share_prefix + share_suffix)
    return combined.astype(jnp.bfloat16).reshape(forks_here, heads_here * V)


MESH = pl.DeviceIdType.MESH


def suffix_fork(i, lens_ref, q_ref, cache_ref, latent_ref, mass_ref):
    positions = lax.broadcasted_iota(jnp.int32, (1, cache_ref.shape[2]), 1)
    live = positions < lens_ref[i]
    scores = jnp.dot(q_ref[i], cache_ref[i], preferred_element_type=jnp.float32)
    scores = jnp.where(live, scores * score_scale, -jnp.inf)
    peak = jnp.max(scores, axis=1, keepdims=True)
    weights = jnp.exp(scores - peak)
    mass = jnp.sum(weights, axis=1, keepdims=True)
    summed = lax.dot_general(
        weights.astype(jnp.bfloat16),
        cache_ref[i, :R, :],
        OUTER,
        preferred_element_type=jnp.float32,
    )
    latent_ref[i] = (summed / mass).astype(jnp.bfloat16)
    mass_ref[i] = jnp.broadcast_to(peak + jnp.log(mass), mass_ref.shape[1:])


def prefix_group(
    slot, first, group, ids_ref, q_ref, cache_ref, latent_ref, mass_ref, out_ref
):
    heads = q_ref.shape[1]
    parts = cache_ref.shape[1]
    ids = [ids_ref[first + i] for i in range(group)]
    rows = jnp.concatenate([q_ref[fork] for fork in ids], axis=0)
    scores = [
        jnp.dot(rows, cache_ref[slot, k], preferred_element_type=jnp.float32)
        for k in range(parts)
    ]
    peak = functools.reduce(
        jnp.maximum, [jnp.max(piece, axis=1, keepdims=True) for piece in scores]
    )
    mass = 0.0
    summed = 0.0
    for k in range(parts):
        weights = jnp.exp2((scores[k] - peak) * (score_scale * log2e))
        mass = mass + jnp.sum(weights, axis=1, keepdims=True)
        summed = summed + lax.dot_general(
            weights.astype(jnp.bfloat16),
            cache_ref[slot, k, :R, :],
            OUTER,
            preferred_element_type=jnp.float32,
        )
    peak = peak * score_scale
    for i, fork in enumerate(ids):
        own = slice(i * heads, (i + 1) * heads)
        other = mass_ref[fork][:, :1]
        top = jnp.maximum(peak[own], other)
        ours = jnp.exp(peak[own] - top)
        theirs = jnp.exp(other - top)
        share = 1.0 / (ours * mass[own] + theirs)
        out_ref[first + i] = (
            summed[own] * (ours * share)
            + latent_ref[fork].astype(jnp.float32) * (theirs * share)
        ).astype(jnp.bfloat16)


def gather_kernel(
    planes,
    steps,
    group,
    lens_ref,
    ids_ref,
    own_ref,
    q_ref,
    suffix_ref,
    packed_ref,
    out_ref,
    latent_ref,
    mass_ref,
    held,
    load_sem,
    own_sem,
    z_send,
    z_recv,
    x_send,
    x_recv,
    y_send,
    y_recv,
    dx_send,
    dx_recv,
    dy_send,
    dy_recv,
    pair_send,
    pair_recv,
):
    dp, tp = lax.axis_index("dp"), lax.axis_index("tp")
    z, x = dp // 2, dp % 2
    y, c = tp // 2, tp % 2
    forks = q_ref.shape[0]
    block = forks // steps
    half = own_ref.shape[1] // 2
    at_x = (z * 2 + (1 - x), tp)
    at_y = (dp, (1 - y) * 2 + c)
    at_pair = (dp, y * 2 + (1 - c))
    at_up = (jnp.minimum(z + 1, planes - 1) * 2 + x, tp)
    at_down = (jnp.maximum(z - 1, 0) * 2 + x, tp)
    has_up, has_down = z + 1 < planes, z > 0

    def place(zz, xx, yy):
        return out_ref.at[zz * 2 + xx, yy * 2 + c]

    def top(ref):
        return ref.at[pl.ds(0, half)]

    def bottom(ref):
        return ref.at[pl.ds(half, half)]

    def copy(src, dst, send, recv, device):
        return pltpu.make_async_remote_copy(
            src_ref=src,
            dst_ref=dst,
            send_sem=send,
            recv_sem=recv,
            device_id=device,
            device_id_type=MESH,
        )

    def z_copy(zz, device, src=None):
        to = place(zz, x, y)
        return copy(to if src is None else src, to, z_send.at[zz], z_recv.at[zz], device)

    def own_up(device, src):
        to = place(z, x, y)
        return copy(src, to, z_send.at[planes], z_recv.at[z], device)

    def x_copy(zz, src=None):
        to = place(zz, x, y)
        return copy(to if src is None else src, to, x_send.at[zz], x_recv.at[zz], at_x)

    def y_copy(zz, src=None):
        to = place(zz, x, y)
        return copy(to if src is None else src, to, y_send.at[zz], y_recv.at[zz], at_y)

    def dy_copy(zz):
        part = top(place(zz, 1 - x, y))
        return copy(part, part, dy_send.at[zz], dy_recv.at[zz], at_y)

    def dx_copy(zz):
        part = bottom(place(zz, x, 1 - y))
        return copy(part, part, dx_send.at[zz], dx_recv.at[zz], at_x)

    def pair_copy(zz, xx, yy, src=None):
        to = place(zz, xx, yy)
        k = (zz * 2 + xx) * 2 + yy
        src = to if src is None else src
        return copy(src, to, pair_send.at[k], pair_recv.at[k], at_pair)

    def load(s):
        part = pl.ds(s * block, block)
        return pltpu.make_async_copy(suffix_ref.at[part], held.at[part], load_sem.at[s])

    for s in range(steps):
        load(s).start()

    barrier = pltpu.get_barrier_semaphore()
    for device in (at_x, at_y, at_pair):
        pl.semaphore_signal(barrier, inc=1, device_id=device, device_id_type=MESH)

    @pl.when(has_up)
    def _():
        pl.semaphore_signal(barrier, inc=1, device_id=at_up, device_id_type=MESH)

    @pl.when(has_down)
    def _():
        pl.semaphore_signal(barrier, inc=1, device_id=at_down, device_id_type=MESH)

    pl.semaphore_wait(barrier, 3 + has_up.astype(jnp.int32) + has_down.astype(jnp.int32))

    mine = own_ref.at[0]

    @pl.when(has_up)
    def _():
        z_copy(z, at_up, mine).start()

    @pl.when(has_down)
    def _():
        own_up(at_down, mine).start()

    x_copy(z, mine).start()
    y_copy(z, mine).start()
    pair_copy(z, x, y, mine).start()
    local = pltpu.make_async_copy(mine, place(z, x, y), own_sem)
    local.start()

    def compute(low, high):
        def step(s, carry):
            load(s).wait()
            for i in range(block):
                suffix_fork(s * block + i, lens_ref, q_ref, held, latent_ref, mass_ref)
            return carry

        lax.fori_loop(low, high, step, 0)

    def arrived(d):
        for sign in (-1, 1):
            zz = z + sign * d
            onward = has_up if sign < 0 else has_down
            device = at_up if sign < 0 else at_down

            @pl.when((zz >= 0) & (zz < planes))
            def _():
                z_copy(zz, device).wait_recv()

                @pl.when(onward)
                def _():
                    z_copy(zz, device).start()

                x_copy(zz).start()
                y_copy(zz).start()
                pair_copy(zz, x, y).start()

    def each(d, act):
        if d == 0:
            act(z)
            return
        for sign in (-1, 1):
            zz = z + sign * d
            pl.when((zz >= 0) & (zz < planes))(functools.partial(act, zz))

    def across(zz):
        x_copy(zz).wait_recv()
        dy_copy(zz).start()
        pair_copy(zz, 1 - x, y).start()
        y_copy(zz).wait_recv()
        dx_copy(zz).start()
        pair_copy(zz, x, 1 - y).start()

    def diagonal(zz):
        dy_copy(zz).wait_recv()
        dx_copy(zz).wait_recv()
        pair_copy(zz, 1 - x, 1 - y).start()

    capacity = packed_ref.shape[0] // (planes * 2)
    groups = capacity // group

    def attend(zz):
        for xx in range(2):
            for yy in range(2):
                pair_copy(zz, xx, yy).wait_recv()

        def one(j, carry):
            slot = zz * 2 + j // groups
            first = slot * capacity + lax.rem(j, groups) * group
            prefix_group(
                slot, first, group, ids_ref, q_ref, out_ref, latent_ref, mass_ref, packed_ref
            )
            return carry

        lax.fori_loop(0, 2 * groups, one, 0)

    marks = [min(steps, 3 * r * steps // 8) for r in range(planes + 1)]
    marks[planes - 1 :] = [steps, steps]
    compute(0, marks[1])
    for r in range(1, planes):
        arrived(r)
        if r < planes - 1:
            each(r - 1, across)
            compute(marks[r], marks[r + 1])
    compute(marks[planes - 1], steps)
    local.wait()
    each(0, diagonal)
    attend(z)
    for r in range(planes - 2, planes):
        each(r, across)
        if r < planes - 1:
            for d in range(1, r):
                each(d, diagonal)
    for d in range(1, planes):
        if d >= planes - 2:
            each(d, diagonal)
        each(d, attend)

    @pl.when(has_down)
    def _():
        own_up(at_down, mine).wait_send()

    for zz in range(planes):
        sent = ((zz <= z) & has_up) | ((zz > z) & has_down)

        @pl.when(sent)
        def _():
            z_copy(zz, at_up).wait_send()

        x_copy(zz).wait_send()
        y_copy(zz).wait_send()
        dx_copy(zz).wait_send()
        dy_copy(zz).wait_send()
        for xx in range(2):
            for yy in range(2):
                pair_copy(zz, xx, yy).wait_send()


def gather_and_attend(
    prefix_cache, query_heads, suffix_cache, suffix_len, ids, steps=8
):
    forks, heads, width = query_heads.shape
    slots, parts = lax.axis_size("dp"), lax.axis_size("tp")
    planes = slots // 2
    group = math.gcd(8, ids.shape[0] // slots)
    dma = pltpu.SemaphoreType.DMA
    smem = pl.BlockSpec(memory_space=pltpu.SMEM)
    vmem = pl.BlockSpec(memory_space=pltpu.VMEM)
    hbm = pl.BlockSpec(memory_space=pl.ANY)
    return pl.pallas_call(
        functools.partial(gather_kernel, planes, steps, group),
        in_specs=[smem, smem, hbm, vmem, hbm],
        out_specs=vmem,
        out_shape=jax.ShapeDtypeStruct((ids.shape[0], heads, R), jnp.bfloat16),
        scratch_shapes=[
            pltpu.VMEM((slots, parts, *prefix_cache.shape[1:]), jnp.bfloat16),
            pltpu.VMEM((forks, heads, R), jnp.bfloat16),
            pltpu.VMEM((forks, heads, 128), jnp.float32),
            pltpu.VMEM(suffix_cache.shape, jnp.bfloat16),
            dma((steps,)),
            dma,
            dma((planes + 1,)),
            *[dma((planes,)) for _ in range(9)],
            dma((slots * 2,)),
            dma((slots * 2,)),
        ],
        compiler_params=pltpu.CompilerParams(
            collective_id=0, has_side_effects=True, vmem_limit_bytes=48 * 1024 * 1024
        ),
        name="gather",
    )(suffix_len, ids, prefix_cache, query_heads, suffix_cache)


def unpack_kernel(target_ref, packed_ref, out_ref):
    for fork in range(out_ref.shape[0]):
        out_ref[fork] = packed_ref[target_ref[fork]]


def unpack(target, packed):
    vmem = pl.BlockSpec(memory_space=pltpu.VMEM)
    return pl.pallas_call(
        unpack_kernel,
        in_specs=[pl.BlockSpec(memory_space=pltpu.SMEM), vmem],
        out_specs=vmem,
        out_shape=jax.ShapeDtypeStruct((target.shape[0], *packed.shape[1:]), packed.dtype),
        name="unpack",
    )(target, packed)


def fork_places(fork_prompt, prompt_slot, slots, capacity):
    forks = fork_prompt.shape[0]
    prompt_ids = jnp.arange(prompt_slot.shape[0], dtype=jnp.int32)
    chosen = fork_prompt[:, 0][:, None] == prompt_ids[None, :]
    owner_slot = jnp.sum(jnp.where(chosen, prompt_slot[None, :], 0), axis=1)
    order = jnp.arange(forks, dtype=jnp.int32)
    before = (owner_slot[:, None] == owner_slot[None, :]) & (order[None, :] < order[:, None])
    target = owner_slot * capacity + jnp.sum(before.astype(jnp.int32), axis=1)
    spots = jnp.arange(slots * capacity, dtype=jnp.int32)
    ids = jnp.sum(jnp.where(target[None, :] == spots[:, None], order[None, :], 0), axis=1)
    return target, ids


def gather_plan(queries, prefix_cache, suffix_cache, w_uv, fork_prompt, prompt_slot, suffix_len):
    forks_here = queries.shape[0]
    heads_here = w_uv.shape[0]
    slots = lax.axis_size("dp")
    capacity = max(2, 2 * forks_here // slots)
    target, ids = fork_places(fork_prompt, prompt_slot, slots, capacity)
    query_heads = queries.reshape(forks_here, heads_here, R + P_SIZE)
    packed = gather_and_attend(prefix_cache, query_heads, suffix_cache, suffix_len, ids)
    latent = unpack(target, packed)
    return project(latent, w_uv).reshape(forks_here, heads_here * V)


def shards(queries, prefix_cache, *others):
    owners_count = lax.axis_size("dp")
    forks_here = queries.shape[0]
    capacity = max(2, 2 * forks_here // owners_count)
    sent = owners_count * capacity * queries.shape[1]
    gathered = owners_count * lax.axis_size("tp") * prefix_cache.size
    square = lax.axis_size("tp") == 4 and owners_count % 2 == 0
    plan = gather_plan if square and gathered <= 4 * sent else exchange_plan
    return plan(queries, prefix_cache, *others)


def solution(mesh):
    placed = (
        P("dp", "tp"),
        P("dp", None, "tp"),
        P("dp", None, None),
        P("tp", None, None),
        P("dp", None),
        P(),
        P("dp"),
    )
    return jax.shard_map(
        shards, mesh=mesh, in_specs=placed, out_specs=P("dp", "tp"), check_vma=False
    )
```
